32 devices in a mesh: dp: 2 (over x), tp: 4 (over z), sp: 4 (over y, core).
Axes of the slice: x: 2, y: 2, z: 4, core: 2. Of those that a mesh axis runs over, the one named last changes fastest.
Arguments:
- hidden: bfloat16 [128, 6144], P('dp'), parts along dimension 0
- norm_scale: bfloat16 [6144], replicated
- w_qkv: bfloat16 [6144, 8192], P(None, 'tp')
- w_out: bfloat16 [6144, 6144], P('tp')
- k_cache: bfloat16 [128, 1024, 8, 128], P('dp', 'sp', 'tp'), parts along dimension 0
- v_cache: bfloat16 [128, 1024, 8, 128], P('dp', 'sp', 'tp'), parts along dimension 0
- positions: int32 [128], P('dp'), parts along dimension 0
Outputs:
- output 1: bfloat16 [128, 6144], P('dp'), parts along dimension 0
- output 2: bfloat16 [128, 1024, 8, 128], P('dp', 'sp', 'tp'), parts along dimension 0
- output 3: bfloat16 [128, 1024, 8, 128], P('dp', 'sp', 'tp'), parts along dimension 0
There are 2 independent parts. The reference program is written for one: setup_inputs(seed, part) draws one part's arguments, and reference() takes and returns one part's arrays. A program takes and returns all parts, laid end to end along the dimension named above; an argument that names none is the same for every part.
All inputs are finite; a program needn't handle non-finite values.
Results may differ from the reference program's by a relative error of at most 0.00644112.
Values sent between devices are 32-bit elements.
A program may use at most 1 GiB of HBM per device.

```python
import math
import jax
import jax.numpy as jnp
from jax import lax

BATCH = 64
SEQ = 1024
D = 6144
HEADS = 48
KV_HEADS = 8
HEAD = 128


def rope_apply(head_vals, positions):
    half_dim = head_vals.shape[-1] // 2
    inv_freq = jnp.exp(jnp.arange(half_dim, dtype=jnp.float32) * (-2.0 * math.log(500000.0) / head_vals.shape[-1]))
    angles = positions.astype(jnp.float32)[:, None] * inv_freq[None, :]
    cos_part = jnp.cos(angles)[:, None, None, :]
    sin_part = jnp.sin(angles)[:, None, None, :]
    first_half = head_vals[..., :half_dim]
    second_half = head_vals[..., half_dim:]
    return jnp.concatenate([first_half * cos_part - second_half * sin_part, second_half * cos_part + first_half * sin_part], axis=-1)


def setup_inputs(seed: int = 0, part: int = 0) -> dict:
    part_keys = jax.random.split(jax.random.fold_in(jax.random.key(seed), part), 5)
    shared_keys = jax.random.split(jax.random.key(seed + 1), 4)
    qkv_width = (HEADS + 2 * KV_HEADS) * HEAD
    hidden = jax.random.normal(part_keys[0], (BATCH, D), jnp.float32)
    norm_scale = 1.0 + 0.5 * jax.random.normal(shared_keys[0], (D,), jnp.float32)
    col_boost = jnp.where(jax.random.randint(shared_keys[1], (qkv_width,), 0, 16) == 0, 10.0, 1.0)
    w_qkv = jax.random.normal(shared_keys[2], (D, qkv_width), jnp.float32) * col_boost * (D ** -0.5)
    w_out = jax.random.normal(shared_keys[3], (HEADS * HEAD, D), jnp.float32) * (2.0 * (HEADS * HEAD) ** -0.5)
    k_cache = 0.5 * jax.random.normal(part_keys[1], (BATCH, SEQ, KV_HEADS, HEAD), jnp.float32)
    coarse = jax.random.normal(part_keys[2], (BATCH, 8, 1, KV_HEADS, HEAD), jnp.float32)
    fine_part = jax.random.normal(part_keys[3], (BATCH, 8, SEQ // 8, KV_HEADS, HEAD), jnp.float32)
    v_cache = (coarse + 0.5 * fine_part).reshape(BATCH, SEQ, KV_HEADS, HEAD)
    positions = jax.random.randint(part_keys[4], (BATCH,), SEQ // 8, SEQ)
    positions = positions.at[0].set(SEQ - 1).at[1].set(SEQ // 8)
    return {
        'hidden': hidden.astype(jnp.bfloat16),
        'norm_scale': norm_scale.astype(jnp.bfloat16),
        'w_qkv': w_qkv.astype(jnp.bfloat16),
        'w_out': w_out.astype(jnp.bfloat16),
        'k_cache': k_cache.astype(jnp.bfloat16),
        'v_cache': v_cache.astype(jnp.bfloat16),
        'positions': positions.astype(jnp.int32),
    }


def reference(hidden, norm_scale, w_qkv, w_out, k_cache, v_cache, positions):
    q_per_kv = HEADS // KV_HEADS
    hidden_f32 = hidden.astype(jnp.float32)
    row_mean = jnp.mean(hidden_f32, axis=-1, keepdims=True)
    centered = hidden_f32 - row_mean
    row_var = jnp.mean(centered * centered, axis=-1, keepdims=True)
    normed = (centered * lax.rsqrt(row_var + 1e-5) * norm_scale.astype(jnp.float32)).astype(jnp.bfloat16)
    qkv_proj = jnp.clip(jnp.dot(normed, w_qkv, preferred_element_type=jnp.float32).astype(jnp.bfloat16), -8.0, 8.0)
    grouped = qkv_proj.reshape(BATCH, KV_HEADS, q_per_kv + 2, HEAD)
    rotated = rope_apply(grouped[:, :, : q_per_kv + 1].astype(jnp.float32), positions).astype(jnp.bfloat16)
    queries = rotated[:, :, :q_per_kv]
    new_row = (jnp.arange(SEQ)[None, :] == positions[:, None])[:, :, None, None]
    k_upd = jnp.where(new_row, rotated[:, :, q_per_kv][:, None], k_cache)
    v_upd = jnp.where(new_row, grouped[:, :, q_per_kv + 1][:, None], v_cache)

    def one_sequence(seq_args):
        q_seq, k_seq, v_seq, p_seq = seq_args
        scores = jnp.einsum('gqd,sgd->gqs', q_seq.astype(jnp.float32), k_seq.astype(jnp.float32)) * (HEAD ** -0.5)
        valid_mask = jnp.arange(SEQ) <= p_seq
        scores = jnp.where(valid_mask[None, None, :], scores, -jnp.inf)
        weights_bf = jax.nn.softmax(scores, axis=-1).astype(jnp.bfloat16)
        return jnp.einsum('gqs,sgd->gqd', weights_bf.astype(jnp.float32), v_seq.astype(jnp.float32))

    attn_out = lax.map(one_sequence, (queries, k_upd, v_upd, positions))
    attn_flat = attn_out.reshape(BATCH, HEADS * HEAD).astype(jnp.bfloat16)
    h_out = (hidden_f32 + jnp.dot(attn_flat, w_out, preferred_element_type=jnp.float32)).astype(jnp.bfloat16)
    return (h_out, k_upd, v_upd)
```

```python
import math
import jax
import jax.numpy as jnp
from jax import lax
from jax.experimental import pallas as pl
from jax.experimental.pallas import tpu as pltpu
from jax.sharding import PartitionSpec as P

F32 = jnp.float32
BF16 = jnp.bfloat16
MESH = pl.DeviceIdType.MESH

NB = 64
D = 6144
HD = 128
SEQ_LOCAL = 256
ROWS = 2 * SEQ_LOCAL
QPK = 6
NEG = -1e30

WCOL = 256
WSLOTS = 4
CB = 8
NCB = NB // CB
VMEM_OUT = True

HALF = 32
NC = 12
CW = D // 2 // NC
SKEW = 3


def attn_kernel(hid, scale, cosf, sinf, pos, w_hbm, k_hbm, v_hbm,
                o_ref, st_ref, k_out, v_out,
                *scratch):
    if VMEM_OUT:
        x_s, wbuf, q_s, kv_s, wsem, ksem, vsem = scratch
        k_ref, v_ref = k_out, v_out
    else:
        x_s, wbuf, q_s, kv_s, wsem, ksem, vsem, k_ref, v_ref, kosem, vosem = scratch
    nw = w_hbm.shape[1] // WCOL
    sp = lax.axis_index('sp')

    def wcopy(j):
        return pltpu.make_async_copy(w_hbm.at[:, pl.ds(pl.multiple_of(j * WCOL, WCOL), WCOL)], wbuf.at[j % WSLOTS], wsem.at[j % WSLOTS])

    def kcopy(c):
        return pltpu.make_async_copy(k_hbm.at[pl.ds(c * CB, CB)], k_ref.at[pl.ds(c * CB, CB)], ksem.at[c])

    def vcopy(c):
        return pltpu.make_async_copy(v_hbm.at[pl.ds(c * CB, CB)], v_ref.at[pl.ds(c * CB, CB)], vsem.at[c])

    for j in range(WSLOTS):
        wcopy(j).start()

    def norm_block(i, carry):
        rows = pl.ds(pl.multiple_of(i * 16, 16), 16)
        h = hid[rows, :].astype(F32)
        mean = jnp.mean(h, axis=-1, keepdims=True)
        cen = h - mean
        var = jnp.mean(cen * cen, axis=-1, keepdims=True)
        x_s[rows, :] = (cen * lax.rsqrt(var + 1e-5) * scale[...].astype(F32)).astype(BF16)
        return carry

    lax.fori_loop(0, NB // 16, norm_block, 0)
    q_s[...] = jnp.zeros_like(q_s)

    def rope(y):
        r = y * cosf[...] + pltpu.roll(y, HD // 2, 1) * sinf[...]
        return r.astype(BF16).astype(F32)

    def group(g, carry):
        for jj in range(4):
            j = g * 4 + jj
            wcopy(j).wait()
            acc = jnp.dot(x_s[...], wbuf[j % WSLOTS], preferred_element_type=F32)

            @pl.when(g == 0)
            def _():
                wcopy(j + WSLOTS).start()

            @pl.when(g == 1)
            def _():
                for c in range(2):
                    kcopy(2 * jj + c).start()
                    vcopy(2 * jj + c).start()

            y = jnp.clip(acc.astype(BF16).astype(F32), -8.0, 8.0)
            y0, y1 = y[:, :HD], y[:, HD:]
            if jj < 3:
                q_s[pl.ds(g * 8 + 2 * jj, NB, stride=16), :] = rope(y0)
                q_s[pl.ds(g * 8 + 2 * jj + 1, NB, stride=16), :] = rope(y1)
            else:
                kv_s[pl.ds(g, NB, stride=8), :] = rope(y0)
                kv_s[pl.ds(g + 2, NB, stride=8), :] = y1
        return carry

    lax.fori_loop(0, 2, group, 0)

    sub16 = lax.broadcasted_iota(jnp.int32, (16, HD), 0)
    col = lax.broadcasted_iota(jnp.int32, (16, ROWS), 1)
    row = lax.broadcasted_iota(jnp.int32, (16, ROWS), 0)
    parity_ok = (col % 2) == (row // 8)
    lane = lax.broadcasted_iota(jnp.int32, (16, HD), 1)

    def insert(b, r, cache, base_row):
        own = jnp.logical_and(r >= 0, r < SEQ_LOCAL)
        rc = jnp.clip(r, 0, SEQ_LOCAL - 1)
        start = pl.multiple_of((rc // 8) * 16, 16)
        sub = jnp.where(own, rc % 8, -1)
        n0 = kv_s[pl.ds(b * 8 + base_row, 1), :]
        n1 = kv_s[pl.ds(b * 8 + base_row + 1, 1), :]
        new = jnp.where(sub16 % 2 == 0, n0, n1)
        tile = cache[b, pl.ds(start, 16), :].astype(F32)
        cache[b, pl.ds(start, 16), :] = jnp.where(sub16 // 2 == sub, new, tile).astype(BF16)

    def chunk(c, stats):
        kcopy(c).wait()
        vcopy(c).wait()
        for i in range(CB):
            b = c * CB + i
            r = pos[b] - sp * SEQ_LOCAL
            insert(b, r, k_ref, 0)
            insert(b, r, v_ref, 2)
        if not VMEM_OUT:
            pltpu.make_async_copy(k_ref.at[pl.ds(c * CB, CB)], k_out.at[pl.ds(c * CB, CB)], kosem.at[c]).start()
            pltpu.make_async_copy(v_ref.at[pl.ds(c * CB, CB)], v_out.at[pl.ds(c * CB, CB)], vosem.at[c]).start()
        for i in range(CB):
            b = c * CB + i
            r = pos[b] - sp * SEQ_LOCAL
            q = q_s[pl.ds(pl.multiple_of(b * 16, 16), 16), :].astype(BF16)
            s = lax.dot_general(q, k_ref[b], (((1,), (1,)), ((), ())), preferred_element_type=F32) * (HD ** -0.5)
            s = jnp.where(jnp.logical_and(parity_ok, col < 2 * r + 2), s, NEG)
            m = jnp.max(s, axis=1, keepdims=True)
            p = jnp.exp(s - m)
            l = jnp.sum(p, axis=1, keepdims=True)
            o = jnp.dot(p.astype(BF16), v_ref[b], preferred_element_type=F32)
            o_ref[pl.ds(b, 16, stride=NB), :] = o
            stats = jnp.where(lane == b, m, jnp.where(lane == b + NB, l, stats))
        return stats

    stats = lax.fori_loop(0, NCB, chunk, jnp.zeros((16, HD), F32))
    for g in range(2):
        block = jnp.concatenate([stats[8 * g:8 * g + 8], jnp.zeros((HD - 8, HD), F32)], axis=0)
        st_ref[g] = jnp.transpose(block).reshape(2, NB, HD)
    if not VMEM_OUT:
        for c in range(NCB):
            pltpu.make_async_copy(k_ref.at[pl.ds(c * CB, CB)], k_out.at[pl.ds(c * CB, CB)], kosem.at[c]).wait()
            pltpu.make_async_copy(v_ref.at[pl.ds(c * CB, CB)], v_out.at[pl.ds(c * CB, CB)], vosem.at[c]).wait()


def merge_kernel(o_in, st_in, hid, w_hbm, out,
                 wbuf, oa, sta, o2, st2, ob, stb, a_own, a_rem, p_s, z1, a_z, z2, t_s, y_in, c_in, cy_in,
                 wsem, osem, s1, r1, s2, r2, s3, r3, zs, zr, z2s, z2r, ts, ys, yr, cs, cr, cys, cyr):
    dp = lax.axis_index('dp')
    tp = lax.axis_index('tp')
    sp = lax.axis_index('sp')
    core = sp % 2
    yy = sp // 2
    partner = sp + 1 - 2 * core
    ynbr = sp + 2 - 4 * yy
    inner = jnp.logical_or(tp == 1, tp == 2)
    outer = jnp.logical_not(inner)
    n_inner = jnp.where(inner, 1, 0)
    z_in_nbr = jnp.where(tp < 2, jnp.where(tp == 0, 1, 2), jnp.where(tp == 3, 2, 1))
    z_out_nbr = jnp.where(tp < 2, 0, 3)

    def dev(t, s):
        return (dp, t, s)

    cols = core * (D // 2)

    def wcopy(j):
        return pltpu.make_async_copy(w_hbm.at[:, pl.ds(pl.multiple_of(cols + j * CW, CW), CW)], wbuf.at[j], wsem.at[j])

    for j in range(NC):
        wcopy(j).start()

    barrier = pltpu.get_barrier_semaphore()
    pl.semaphore_signal(barrier, inc=1, device_id=dev(tp, partner), device_id_type=MESH)
    pl.semaphore_signal(barrier, inc=1, device_id=dev(tp, ynbr), device_id_type=MESH)
    pl.semaphore_signal(barrier, inc=1, device_id=dev(z_in_nbr, sp), device_id_type=MESH)

    @pl.when(inner)
    def _():
        pl.semaphore_signal(barrier, inc=1, device_id=dev(z_out_nbr, sp), device_id_type=MESH)

    pl.semaphore_wait(barrier, 3 + n_inner)

    def rcopy(src, dst, ssem, rsem, t, s):
        return pltpu.make_async_remote_copy(src_ref=src, dst_ref=dst, send_sem=ssem, recv_sem=rsem, device_id=dev(t, s), device_id_type=MESH)

    ca = rcopy(o_in.at[1 - core, pl.ds(0, QPK)], oa, s1.at[0], r1.at[0], tp, partner)
    cb = rcopy(st_in.at[1 - core], sta, s1.at[1], r1.at[1], tp, partner)
    ca.start()
    cb.start()
    ca.wait_recv()
    cb.wait_recv()

    def factors(m0, l0, m1, l1):
        top = jnp.maximum(m0, m1)
        f0 = jnp.exp(m0 - top)
        f1 = jnp.exp(m1 - top)
        return top, f0, f1, f0 * l0 + f1 * l1

    def pair_merge(start):
        rows = pl.ds(pl.multiple_of(start, HALF), HALF)
        top, f0, f1, total = factors(st_in[core, 0, rows, :], st_in[core, 1, rows, :], sta[0, rows, :], sta[1, rows, :])
        st2[0, rows, :] = top
        st2[1, rows, :] = total
        for i in range(QPK):
            o2[i, rows, :] = o_in[core, i, rows, :] * f0[:, i:i + 1] + oa[i, rows, :] * f1[:, i:i + 1]

    other = pl.ds(pl.multiple_of((1 - yy) * HALF, HALF), HALF)
    mine = pl.ds(pl.multiple_of(yy * HALF, HALF), HALF)
    pair_merge((1 - yy) * HALF)
    cc = rcopy(o2.at[:, other, :], ob, s2.at[0], r2.at[0], tp, ynbr)
    cd = rcopy(st2.at[:, other, :], stb, s2.at[1], r2.at[1], tp, ynbr)
    cc.start()
    cd.start()
    pair_merge(yy * HALF)
    cc.wait_recv()
    cd.wait_recv()
    top, f0, f1, total = factors(st2[0, mine, :], st2[1, mine, :], stb[0], stb[1])
    inv = 1.0 / total
    f0 = f0 * inv
    f1 = f1 * inv
    for i in range(QPK):
        a = o2[i, mine, :] * f0[:, i:i + 1] + ob[i] * f1[:, i:i + 1]
        a_own[i] = a.astype(BF16).astype(F32)
    ce = rcopy(a_own, a_rem, s3, r3, tp, partner)
    ce.start()

    def lhs(ref):
        return jnp.concatenate([ref[i].astype(BF16) for i in range(QPK)], axis=1)

    gk = QPK * HD
    own = lhs(a_own)

    def first(j, carry):
        wcopy(j).wait()
        p_s[j] = jnp.dot(own, wbuf[j, pl.ds(pl.multiple_of(core * gk, gk), gk), :], preferred_element_type=F32)
        return carry

    lax.fori_loop(0, NC, first, 0)
    ce.wait_recv()
    rem = lhs(a_rem)

    def zc(j):
        return rcopy(p_s.at[j], z1.at[j], zs.at[j], zr.at[j], z_in_nbr, sp)

    def second(j, carry):
        p_s[j] += jnp.dot(rem, wbuf[j, pl.ds(pl.multiple_of((1 - core) * gk, gk), gk), :], preferred_element_type=F32)

        @pl.when(outer)
        def _():
            zc(j).start()
        return carry

    lax.fori_loop(0, NC, second, 0)

    def mid(j):
        return rcopy(a_z.at[j], z2.at[j], z2s.at[j], z2r.at[j], z_in_nbr, sp)

    def back(j):
        return rcopy(t_s.at[j], z1.at[j], ts.at[j], zr.at[j], z_out_nbr, sp)

    def ycopy(src, j):
        return rcopy(src.at[j], y_in.at[j], ys.at[j], yr.at[j], tp, ynbr)

    def ccopy(src, j):
        return rcopy(src.at[j], c_in.at[j], cs.at[j], cr.at[j], tp, partner)

    def cycopy(j):
        return rcopy(y_in.at[j], cy_in.at[j], cys.at[j], cyr.at[j], tp, partner)

    def put(rows_start, col_start, j, val):
        rows = pl.ds(pl.multiple_of(rows_start, HALF), HALF)
        cl = pl.ds(pl.multiple_of(col_start + j * CW, CW), CW)
        out[rows, cl] = (hid[rows, cl].astype(F32) + val).astype(BF16)

    ocols = (1 - core) * (D // 2)

    def e3(j):
        ycopy(t_s, j).wait_recv()
        cycopy(j).start()
        put((1 - yy) * HALF, cols, j, y_in[j])

    def e4(j):
        ccopy(t_s, j).wait_recv()
        put(yy * HALF, ocols, j, c_in[j])

    def e5(j):
        cycopy(j).wait_recv()
        put((1 - yy) * HALF, ocols, j, cy_in[j])

    def within(j, fn):
        @pl.when(jnp.logical_and(j >= 0, j < NC))
        def _():
            fn(j)

    @pl.when(inner)
    def _():
        def e1(j):
            back(j).wait_recv()
            a_z[j] = p_s[j] + z1[j]
            mid(j).start()

        def e2(j):
            mid(j).wait_recv()
            t_s[j] = a_z[j] + z2[j]
            back(j).start()
            ycopy(t_s, j).start()
            ccopy(t_s, j).start()
            put(yy * HALF, cols, j, t_s[j])

        def step(t, carry):
            within(t, e1)
            within(t - SKEW, e2)
            within(t - 2 * SKEW, e3)
            within(t - 3 * SKEW, e4)
            within(t - 3 * SKEW, e5)
            return carry

        lax.fori_loop(0, NC + 3 * SKEW, step, 0)

        def drain(j, carry):
            mid(j).wait_send()
            back(j).wait_send()
            ycopy(t_s, j).wait_send()
            ccopy(t_s, j).wait_send()
            cycopy(j).wait_send()
            return carry

        lax.fori_loop(0, NC, drain, 0)

    @pl.when(outer)
    def _():
        def e1(j):
            zc(j).wait_recv()
            ycopy(z1, j).start()
            ccopy(z1, j).start()
            put(yy * HALF, cols, j, z1[j])

        def step(t, carry):
            within(t, e1)
            within(t - SKEW, e3)
            within(t - 2 * SKEW, e4)
            within(t - 2 * SKEW, e5)
            return carry

        lax.fori_loop(0, NC + 2 * SKEW, step, 0)

        def drain(j, carry):
            zc(j).wait_send()
            ycopy(z1, j).wait_send()
            ccopy(z1, j).wait_send()
            cycopy(j).wait_send()
            return carry

        lax.fori_loop(0, NC, drain, 0)

    ca.wait_send()
    cb.wait_send()
    cc.wait_send()
    cd.wait_send()
    ce.wait_send()


def solution(mesh):
    cache_spec = P('dp', 'sp', 'tp', None)
    any_spec = pl.BlockSpec(memory_space=pl.ANY)
    vmem_spec = pl.BlockSpec(memory_space=pltpu.VMEM)
    smem_spec = pl.BlockSpec(memory_space=pltpu.SMEM)
    dma = pltpu.SemaphoreType.DMA

    def local_step(hidden, norm_scale, w_qkv, w_out, k_cache, v_cache, positions):
        inv_freq = jnp.exp(jnp.arange(HD // 2, dtype=F32) * (-2.0 * math.log(500000.0) / HD))
        angles = positions.astype(F32)[:, None] * inv_freq[None, :]
        cos = jnp.cos(angles)
        sin = jnp.sin(angles)
        cosf = jnp.concatenate([cos, cos], axis=1)
        sinf = jnp.concatenate([-sin, sin], axis=1)
        cache_shape = (NB, ROWS, HD)
        if VMEM_OUT:
            cache_out = pltpu.VMEM(cache_shape, BF16)
            cache_out_spec = vmem_spec
            extra = []
        else:
            cache_out = jax.ShapeDtypeStruct(cache_shape, BF16)
            cache_out_spec = any_spec
            extra = [pltpu.VMEM(cache_shape, BF16), pltpu.VMEM(cache_shape, BF16), dma((NCB,)), dma((NCB,))]
        o, st, k_new, v_new = pl.pallas_call(
            attn_kernel,
            out_shape=(jax.ShapeDtypeStruct((16 * NB, HD), F32), jax.ShapeDtypeStruct((2, 2, NB, HD), F32), cache_out, cache_out),
            in_specs=[vmem_spec, vmem_spec, vmem_spec, vmem_spec, smem_spec, any_spec, any_spec, any_spec],
            out_specs=(vmem_spec, vmem_spec, cache_out_spec, cache_out_spec),
            scratch_shapes=[
                pltpu.VMEM((NB, D), BF16),
                pltpu.VMEM((WSLOTS, D, WCOL), BF16),
                pltpu.VMEM((16 * NB, HD), F32),
                pltpu.VMEM((8 * NB, HD), F32),
                dma((WSLOTS,)), dma((NCB,)), dma((NCB,)),
            ] + extra,
            compiler_params=pltpu.CompilerParams(vmem_limit_bytes=(36 << 20) if VMEM_OUT else (56 << 20)),
            cost_estimate=pl.CostEstimate(flops=2 * NB * D * 2048 + 4 * NB * 16 * ROWS * HD, bytes_accessed=60 << 20, transcendentals=NB * 16 * ROWS),
            name='qkv_attention',
        )(hidden, norm_scale.reshape(1, D), cosf, sinf, positions, w_qkv, k_cache.reshape(cache_shape), v_cache.reshape(cache_shape))

        chunk = (NC, HALF, CW)
        h_out = pl.pallas_call(
            merge_kernel,
            out_shape=jax.ShapeDtypeStruct((NB, D), BF16),
            in_specs=[vmem_spec, vmem_spec, vmem_spec, any_spec],
            out_specs=vmem_spec,
            scratch_shapes=[
                pltpu.VMEM((NC, 2 * QPK * HD, CW), BF16),
                pltpu.VMEM((QPK, NB, HD), F32),
                pltpu.VMEM((2, NB, HD), F32),
                pltpu.VMEM((QPK, NB, HD), F32),
                pltpu.VMEM((2, NB, HD), F32),
                pltpu.VMEM((QPK, HALF, HD), F32),
                pltpu.VMEM((2, HALF, HD), F32),
                pltpu.VMEM((QPK, HALF, HD), F32),
                pltpu.VMEM((QPK, HALF, HD), F32),
            ] + [pltpu.VMEM(chunk, F32)] * 8 + [
                dma((NC,)), dma((1,)), dma((2,)), dma((2,)), dma((2,)), dma((2,)), dma(()), dma(()),
            ] + [dma((NC,))] * 11,
            compiler_params=pltpu.CompilerParams(collective_id=0, has_side_effects=True, vmem_limit_bytes=24 << 20),
            cost_estimate=pl.CostEstimate(flops=40_000_000_000, bytes_accessed=12 << 20, transcendentals=0),
            name='merge_project',
        )(o.reshape(2, 8, NB, HD), st, hidden, w_out)
        return h_out, k_new.reshape(k_cache.shape), v_new.reshape(v_cache.shape)

    return jax.shard_map(
        local_step,
        mesh=mesh,
        in_specs=(P('dp', None), P(None), P(None, 'tp'), P('tp', None), cache_spec, cache_spec, P('dp')),
        out_specs=(P('dp', None), cache_spec, cache_spec),
        check_vma=False,
    )
```

```python
import math
import jax
import jax.numpy as jnp
from jax import lax
from jax.experimental import pallas as pl
from jax.experimental.pallas import tpu as pltpu
from jax.sharding import PartitionSpec as P

F32 = jnp.float32
BF16 = jnp.bfloat16
MESH = pl.DeviceIdType.MESH

NB = 64
D = 6144
HD = 128
SEQ_LOCAL = 256
ROWS = 2 * SEQ_LOCAL
QPK = 6
NEG = -1e30

WCOL = 256
WSLOTS = 4
CB = 8
NCB = NB // CB

HALF = 32
CW = 512
WC = 512
NW = (7, 5)
WPW = WC // CW
NC = NW[0] * WPW
SKEW = 2
PIECE = 2
NP = QPK // PIECE


def attn_kernel(pos_hbm, scale_hbm, hid_hbm, w_hbm, k_hbm, v_hbm,
                o_ref, st_ref, k_out, v_out,
                pos, scale, hid, cosf, sinf, x_s, wbuf, q_s, kv_s, k_ref, v_ref, psem, hsem, wsem, ksem, vsem, kosem, vosem):
    sp = lax.axis_index('sp')

    def wcopy(j):
        return pltpu.make_async_copy(w_hbm.at[:, pl.ds(pl.multiple_of(j * WCOL, WCOL), WCOL)], wbuf.at[j % WSLOTS], wsem.at[j % WSLOTS])

    def kcopy(c):
        return pltpu.make_async_copy(k_hbm.at[pl.ds(c * CB, CB)], k_ref.at[pl.ds(c * CB, CB)], ksem.at[c])

    def vcopy(c):
        return pltpu.make_async_copy(v_hbm.at[pl.ds(c * CB, CB)], v_ref.at[pl.ds(c * CB, CB)], vsem.at[c])

    hcopy = pltpu.make_async_copy(hid_hbm, hid, hsem)
    hcopy.start()
    pcopy = pltpu.make_async_copy(pos_hbm, pos, psem.at[0])
    pcopy.start()
    scopy = pltpu.make_async_copy(scale_hbm, scale, psem.at[1])
    scopy.start()
    wcopy(0).start()
    wcopy(1).start()
    pcopy.wait()

    lane8 = lax.broadcasted_iota(jnp.int32, (8, HD), 1)
    sub8 = lax.broadcasted_iota(jnp.int32, (8, HD), 0)
    inv_freq = jnp.exp((lane8 % (HD // 2)).astype(F32) * (-2.0 * math.log(500000.0) / HD))

    def angle_block(i, carry):
        p = jnp.zeros((8, HD), jnp.int32)
        for e in range(8):
            p = jnp.where(sub8 == e, pos[i * 8 + e], p)
        angles = p.astype(F32) * inv_freq
        rows = pl.ds(pl.multiple_of(i * 8, 8), 8)
        cosf[rows, :] = jnp.cos(angles)
        sin = jnp.sin(angles)
        sinf[rows, :] = jnp.where(lane8 < HD // 2, -sin, sin)
        return carry

    lax.fori_loop(0, NB // 8, angle_block, 0)
    q_s[...] = jnp.zeros_like(q_s)
    wcopy(2).start()
    wcopy(3).start()
    hcopy.wait()
    scopy.wait()
    for c in range(2):
        kcopy(c).start()
        vcopy(c).start()

    def norm_block(i, carry):
        rows = pl.ds(pl.multiple_of(i * 16, 16), 16)
        h = hid[rows, :].astype(F32)
        mean = jnp.mean(h, axis=-1, keepdims=True)
        cen = h - mean
        var = jnp.mean(cen * cen, axis=-1, keepdims=True)
        x_s[rows, :] = (cen * lax.rsqrt(var + 1e-5) * scale[...].astype(F32)[None, :]).astype(BF16)
        return carry

    lax.fori_loop(0, NB // 16, norm_block, 0)

    def rope(y):
        r = y * cosf[...] + pltpu.roll(y, HD // 2, 1) * sinf[...]
        return r.astype(BF16).astype(F32)

    def group(g, carry):
        for jj in range(4):
            j = g * 4 + jj
            wcopy(j).wait()
            acc = jnp.dot(x_s[...], wbuf[j % WSLOTS], preferred_element_type=F32)

            @pl.when(g == 0)
            def _():
                wcopy(j + WSLOTS).start()

            @pl.when(g == 1)
            def _():
                for c in range((2, 4, 5, 6)[jj], (4, 5, 6, 8)[jj]):
                    kcopy(c).start()
                    vcopy(c).start()

            y = jnp.clip(acc.astype(BF16).astype(F32), -8.0, 8.0)
            y0, y1 = y[:, :HD], y[:, HD:]
            if jj < 3:
                q_s[pl.ds(g * 8 + 2 * jj, NB, stride=16), :] = rope(y0)
                q_s[pl.ds(g * 8 + 2 * jj + 1, NB, stride=16), :] = rope(y1)
            else:
                kv_s[pl.ds(g, NB, stride=8), :] = rope(y0)
                kv_s[pl.ds(g + 2, NB, stride=8), :] = y1
        return carry

    lax.fori_loop(0, 2, group, 0)

    sub16 = lax.broadcasted_iota(jnp.int32, (16, HD), 0)
    col = lax.broadcasted_iota(jnp.int32, (16, ROWS), 1)
    row = lax.broadcasted_iota(jnp.int32, (16, ROWS), 0)
    parity_ok = (col % 2) == (row // 8)
    lane = lax.broadcasted_iota(jnp.int32, (16, HD), 1)

    def insert(b, r, cache, base_row):
        own = jnp.logical_and(r >= 0, r < SEQ_LOCAL)
        rc = jnp.clip(r, 0, SEQ_LOCAL - 1)
        start = pl.multiple_of((rc // 8) * 16, 16)
        sub = jnp.where(own, rc % 8, -1)
        n0 = kv_s[pl.ds(b * 8 + base_row, 1), :]
        n1 = kv_s[pl.ds(b * 8 + base_row + 1, 1), :]
        new = jnp.where(sub16 % 2 == 0, n0, n1)
        tile = cache[b, pl.ds(start, 16), :].astype(F32)
        cache[b, pl.ds(start, 16), :] = jnp.where(sub16 // 2 == sub, new, tile).astype(BF16)

    def chunk(c, stats):
        kcopy(c).wait()
        vcopy(c).wait()

        for i in range(CB):
            b = c * CB + i
            r = pos[b] - sp * SEQ_LOCAL
            insert(b, r, k_ref, 0)
            insert(b, r, v_ref, 2)
        pltpu.make_async_copy(k_ref.at[pl.ds(c * CB, CB)], k_out.at[pl.ds(c * CB, CB)], kosem.at[c]).start()
        pltpu.make_async_copy(v_ref.at[pl.ds(c * CB, CB)], v_out.at[pl.ds(c * CB, CB)], vosem.at[c]).start()
        scores = []
        for i in range(CB):
            b = c * CB + i
            q = q_s[pl.ds(pl.multiple_of(b * 16, 16), 16), :].astype(BF16)
            scores.append(lax.dot_general(q, k_ref[b], (((1,), (1,)), ((), ())), preferred_element_type=F32) * (HD ** -0.5))
        parts = []
        for i in range(CB):
            r = pos[c * CB + i] - sp * SEQ_LOCAL
            s = jnp.where(jnp.logical_and(parity_ok, col < 2 * r + 2), scores[i], NEG)
            m = jnp.max(s, axis=1, keepdims=True)
            p = jnp.exp(s - m)
            parts.append((m, jnp.sum(p, axis=1, keepdims=True), p.astype(BF16)))
        for i in range(CB):
            b = c * CB + i
            m, l, p = parts[i]
            o_ref[pl.ds(b, 16, stride=NB), :] = jnp.dot(p, v_ref[b], preferred_element_type=F32)
            stats = jnp.where(lane == b, m, jnp.where(lane == b + NB, l, stats))
        return stats

    stats = lax.fori_loop(0, NCB, chunk, jnp.zeros((16, HD), F32))
    for g in range(2):
        block = jnp.concatenate([stats[8 * g:8 * g + 8], jnp.zeros((HD - 8, HD), F32)], axis=0)
        st_ref[g] = jnp.transpose(block).reshape(2, NB, HD)
    for c in range(NCB):
        pltpu.make_async_copy(k_ref.at[pl.ds(c * CB, CB)], k_out.at[pl.ds(c * CB, CB)], kosem.at[c]).wait()
        pltpu.make_async_copy(v_ref.at[pl.ds(c * CB, CB)], v_out.at[pl.ds(c * CB, CB)], vosem.at[c]).wait()


def merge_kernel(o_in, st_in, hid_hbm, w_hbm, out,
                 hid, wbuf, oa, sta, o2, st2, ob, stb, a_own, a_rem, p_s, z1, a_z, z2, t_s, y_in, c_in, cy_in,
                 hsem, wsem, s1, r1, s2, r2, s3, r3, zs, zr, z2s, z2r, ts, ys, yr, cs, cr, cys, cyr):
    dp = lax.axis_index('dp')
    tp = lax.axis_index('tp')
    sp = lax.axis_index('sp')
    core = sp % 2
    yy = sp // 2
    partner = sp + 1 - 2 * core
    ynbr = sp + 2 - 4 * yy
    inner = jnp.logical_or(tp == 1, tp == 2)
    outer = jnp.logical_not(inner)
    n_inner = jnp.where(inner, 1, 0)
    z_in_nbr = jnp.where(tp < 2, jnp.where(tp == 0, 1, 2), jnp.where(tp == 3, 2, 1))
    z_out_nbr = jnp.where(tp < 2, 0, 3)
    nw = jnp.where(core == 1, NW[0], NW[1])
    nc = nw * WPW
    ncp = (NW[0] + NW[1]) * WPW - nc
    cols = jnp.where(core == 1, 0, NW[0] * WC)
    ocols = jnp.where(core == 1, NW[0] * WC, 0)

    def dev(t, s):
        return (dp, t, s)

    barrier = pltpu.get_barrier_semaphore()
    pl.semaphore_signal(barrier, inc=1, device_id=dev(tp, partner), device_id_type=MESH)
    pl.semaphore_signal(barrier, inc=1, device_id=dev(tp, ynbr), device_id_type=MESH)
    pl.semaphore_signal(barrier, inc=1, device_id=dev(z_in_nbr, sp), device_id_type=MESH)

    @pl.when(inner)
    def _():
        pl.semaphore_signal(barrier, inc=1, device_id=dev(z_out_nbr, sp), device_id_type=MESH)

    def wcopy(j):
        return pltpu.make_async_copy(w_hbm.at[:, pl.ds(pl.multiple_of(cols + j * WC, WC), WC)], wbuf.at[j], wsem.at[j])

    def wstart(j, carry):
        wcopy(j).start()
        return carry

    lax.fori_loop(0, nw, wstart, 0)
    hcopy = pltpu.make_async_copy(hid_hbm, hid, hsem)
    hcopy.start()
    pl.semaphore_wait(barrier, 3 + n_inner)

    def rcopy(src, dst, ssem, rsem, t, s):
        return pltpu.make_async_remote_copy(src_ref=src, dst_ref=dst, send_sem=ssem, recv_sem=rsem, device_id=dev(t, s), device_id_type=MESH)

    other = pl.ds(pl.multiple_of((1 - yy) * HALF, HALF), HALF)
    mine = pl.ds(pl.multiple_of(yy * HALF, HALF), HALF)

    cb = rcopy(st_in.at[1 - core], sta, s1.at[NP], r1.at[NP], tp, partner)
    ca = [rcopy(o_in.at[1 - core, pl.ds(i * PIECE, PIECE)], oa.at[pl.ds(i * PIECE, PIECE)], s1.at[i], r1.at[i], tp, partner) for i in range(NP)]
    cb.start()
    for c in ca:
        c.start()
    cd = rcopy(st2.at[:, other, :], stb, s2.at[NP], r2.at[NP], tp, ynbr)
    cc = [rcopy(o2.at[pl.ds(i * PIECE, PIECE), other, :], ob.at[pl.ds(i * PIECE, PIECE)], s2.at[i], r2.at[i], tp, ynbr) for i in range(NP)]
    ce = [rcopy(a_own.at[pl.ds(i * PIECE, PIECE)], a_rem.at[pl.ds(i * PIECE, PIECE)], s3.at[i], r3.at[i], tp, partner) for i in range(NP)]

    def factors(m0, l0, m1, l1):
        top = jnp.maximum(m0, m1)
        f0 = jnp.exp(m0 - top)
        f1 = jnp.exp(m1 - top)
        return top, f0, f1, f0 * l0 + f1 * l1

    def pair_factors(rows):
        top, f0, f1, total = factors(st_in[core, 0, rows, :], st_in[core, 1, rows, :], sta[0, rows, :], sta[1, rows, :])
        st2[0, rows, :] = top
        st2[1, rows, :] = total
        return f0, f1

    def pair_merge(i, rows, f0, f1):
        o2[i, rows, :] = o_in[core, i, rows, :] * f0[:, i:i + 1] + oa[i, rows, :] * f1[:, i:i + 1]

    cb.wait_recv()
    f0, f1 = pair_factors(other)
    cd.start()
    for i in range(NP):
        ca[i].wait_recv()
        for h in range(i * PIECE, (i + 1) * PIECE):
            pair_merge(h, other, f0, f1)
        cc[i].start()
    f0, f1 = pair_factors(mine)
    for h in range(QPK):
        pair_merge(h, mine, f0, f1)
    cd.wait_recv()
    top, f0, f1, total = factors(st2[0, mine, :], st2[1, mine, :], stb[0], stb[1])
    inv = 1.0 / total
    f0 = f0 * inv
    f1 = f1 * inv
    for i in range(NP):
        cc[i].wait_recv()
        for h in range(i * PIECE, (i + 1) * PIECE):
            a = o2[h, mine, :] * f0[:, h:h + 1] + ob[h] * f1[:, h:h + 1]
            a_own[h] = a.astype(BF16).astype(F32)
        ce[i].start()

    def lhs(ref):
        return jnp.concatenate([ref[i].astype(BF16) for i in range(QPK)], axis=1)

    gk = QPK * HD
    own_rows = pl.ds(pl.multiple_of(core * gk, gk), gk)
    rem_rows = pl.ds(pl.multiple_of((1 - core) * gk, gk), gk)
    own = lhs(a_own)

    def first(j, carry):
        wcopy(j).wait()
        p = jnp.dot(own, wbuf[j, own_rows, :], preferred_element_type=F32)
        for e in range(WPW):
            p_s[j * WPW + e] = p[:, e * CW:(e + 1) * CW]
        return carry

    lax.fori_loop(0, nw, first, 0)
    for c in ce:
        c.wait_recv()
    rem = lhs(a_rem)

    def zc(j):
        return rcopy(p_s.at[j], z1.at[j], zs.at[j], zr.at[j], z_in_nbr, sp)

    def second(j, carry):
        p = jnp.dot(rem, wbuf[j, rem_rows, :], preferred_element_type=F32)
        for e in range(WPW):
            p_s[j * WPW + e] += p[:, e * CW:(e + 1) * CW]

        @pl.when(outer)
        def _():
            for e in range(WPW):
                zc(j * WPW + e).start()
        return carry

    lax.fori_loop(0, nw, second, 0)
    hcopy.wait()

    def mid(j):
        return rcopy(a_z.at[j], z2.at[j], z2s.at[j], z2r.at[j], z_in_nbr, sp)

    def back(j):
        return rcopy(t_s.at[j], z1.at[j], ts.at[j], zr.at[j], z_out_nbr, sp)

    def ycopy(src, j):
        return rcopy(src.at[j], y_in.at[j], ys.at[j], yr.at[j], tp, ynbr)

    def ccopy(src, j):
        return rcopy(src.at[j], c_in.at[j], cs.at[j], cr.at[j], tp, partner)

    def cycopy(j):
        return rcopy(y_in.at[j], cy_in.at[j], cys.at[j], cyr.at[j], tp, partner)

    def put(rows_start, col_start, j, val):
        rows = pl.ds(pl.multiple_of(rows_start, HALF), HALF)
        cl = pl.ds(pl.multiple_of(col_start + j * CW, CW), CW)
        out[rows, cl] = (hid[rows, cl].astype(F32) + val).astype(BF16)

    def e3(j):
        ycopy(t_s, j).wait_recv()
        cycopy(j).start()
        put((1 - yy) * HALF, cols, j, y_in[j])

    def e4(j):
        ccopy(t_s, j).wait_recv()
        put(yy * HALF, ocols, j, c_in[j])

    def e5(j):
        cycopy(j).wait_recv()
        put((1 - yy) * HALF, ocols, j, cy_in[j])

    def within(j, n, fn):
        @pl.when(jnp.logical_and(j >= 0, j < n))
        def _():
            fn(j)

    def tail(j, carry):
        e4(j)
        e5(j)
        return carry

    @pl.when(inner)
    def _():
        def e1(j):
            back(j).wait_recv()
            a_z[j] = p_s[j] + z1[j]
            mid(j).start()

        def e2(j):
            mid(j).wait_recv()
            t_s[j] = a_z[j] + z2[j]
            back(j).start()
            ycopy(t_s, j).start()
            ccopy(t_s, j).start()
            put(yy * HALF, cols, j, t_s[j])

        def step(t, carry):
            within(t, nc, e1)
            within(t - SKEW, nc, e2)
            within(t - 2 * SKEW, nc, e3)
            return carry

        lax.fori_loop(0, nc + 2 * SKEW, step, 0)
        lax.fori_loop(0, ncp, tail, 0)

        def drain(j, carry):
            mid(j).wait_send()
            back(j).wait_send()
            ycopy(t_s, j).wait_send()
            ccopy(t_s, j).wait_send()
            cycopy(j).wait_send()
            return carry

        lax.fori_loop(0, nc, drain, 0)

    @pl.when(outer)
    def _():
        def e1(j):
            zc(j).wait_recv()
            ycopy(z1, j).start()
            ccopy(z1, j).start()
            put(yy * HALF, cols, j, z1[j])

        def step(t, carry):
            within(t, nc, e1)
            within(t - SKEW, nc, e3)
            return carry

        lax.fori_loop(0, nc + SKEW, step, 0)
        lax.fori_loop(0, ncp, tail, 0)

        def drain(j, carry):
            zc(j).wait_send()
            ycopy(z1, j).wait_send()
            ccopy(z1, j).wait_send()
            cycopy(j).wait_send()
            return carry

        lax.fori_loop(0, nc, drain, 0)

    for c in ca + cc + ce + [cb, cd]:
        c.wait_send()


def solution(mesh):
    cache_spec = P('dp', 'sp', 'tp', None)
    any_spec = pl.BlockSpec(memory_space=pltpu.HBM)
    vmem_spec = pl.BlockSpec(memory_space=pltpu.VMEM)
    dma = pltpu.SemaphoreType.DMA

    def in_hbm(x):
        return pltpu.with_memory_space_constraint(x, pltpu.HBM)

    def local_step(hidden, norm_scale, w_qkv, w_out, k_cache, v_cache, positions):
        cache_shape = (NB, ROWS, HD)
        cache_out = jax.ShapeDtypeStruct(cache_shape, BF16)
        o, st, k_new, v_new = pl.pallas_call(
            attn_kernel,
            out_shape=(jax.ShapeDtypeStruct((16 * NB, HD), F32), jax.ShapeDtypeStruct((2, 2, NB, HD), F32), cache_out, cache_out),
            in_specs=[any_spec] * 6,
            out_specs=(vmem_spec, vmem_spec, any_spec, any_spec),
            scratch_shapes=[
                pltpu.SMEM((NB,), jnp.int32),
                pltpu.VMEM((D,), BF16),
                pltpu.VMEM((NB, D), BF16),
                pltpu.VMEM((NB, HD), F32),
                pltpu.VMEM((NB, HD), F32),
                pltpu.VMEM((NB, D), BF16),
                pltpu.VMEM((WSLOTS, D, WCOL), BF16),
                pltpu.VMEM((16 * NB, HD), F32),
                pltpu.VMEM((8 * NB, HD), F32),
                pltpu.VMEM(cache_shape, BF16),
                pltpu.VMEM(cache_shape, BF16),
                dma((2,)), dma(()), dma((WSLOTS,)), dma((NCB,)), dma((NCB,)), dma((NCB,)), dma((NCB,)),
            ],
            compiler_params=pltpu.CompilerParams(vmem_limit_bytes=46 << 20),
            name='qkv_attention',
        )(in_hbm(positions), in_hbm(norm_scale), in_hbm(hidden), in_hbm(w_qkv), in_hbm(k_cache.reshape(cache_shape)), in_hbm(v_cache.reshape(cache_shape)))

        chunk = (NC, HALF, CW)
        h_out = pl.pallas_call(
            merge_kernel,
            out_shape=jax.ShapeDtypeStruct((NB, D), BF16),
            in_specs=[vmem_spec, vmem_spec, any_spec, any_spec],
            out_specs=vmem_spec,
            scratch_shapes=[
                pltpu.VMEM((NB, D), BF16),
                pltpu.VMEM((NW[0], 2 * QPK * HD, WC), BF16),
                pltpu.VMEM((QPK, NB, HD), F32),
                pltpu.VMEM((2, NB, HD), F32),
                pltpu.VMEM((QPK, NB, HD), F32),
                pltpu.VMEM((2, NB, HD), F32),
                pltpu.VMEM((QPK, HALF, HD), F32),
                pltpu.VMEM((2, HALF, HD), F32),
                pltpu.VMEM((QPK, HALF, HD), F32),
                pltpu.VMEM((QPK, HALF, HD), F32),
            ] + [pltpu.VMEM(chunk, F32)] * 8 + [
                dma(()), dma((NW[0],)), dma((NP + 1,)), dma((NP + 1,)), dma((NP + 1,)), dma((NP + 1,)), dma((NP,)), dma((NP,)),
            ] + [dma((NC,))] * 11,
            compiler_params=pltpu.CompilerParams(collective_id=0, has_side_effects=True, vmem_limit_bytes=32 << 20),
            name='merge_project',
        )(o.reshape(2, 8, NB, HD), st, in_hbm(hidden), in_hbm(w_out))
        return h_out, k_new.reshape(k_cache.shape), v_new.reshape(v_cache.shape)

    return jax.shard_map(
        local_step,
        mesh=mesh,
        in_specs=(P('dp', None), P(None), P(None, 'tp'), P('tp', None), cache_spec, cache_spec, P('dp')),
        out_specs=(P('dp', None), cache_spec, cache_spec),
        check_vma=False,
    )
```

```python
import math
import jax
import jax.numpy as jnp
from jax import lax
from jax.experimental import pallas as pl
from jax.experimental.pallas import tpu as pltpu
from jax.sharding import PartitionSpec as P

F32 = jnp.float32
BF16 = jnp.bfloat16
MESH = pl.DeviceIdType.MESH

NB = 64
D = 6144
HD = 128
SEQ_LOCAL = 256
ROWS = 2 * SEQ_LOCAL
QPK = 6
NEG = -1e30

WCOL = 256
WSLOTS = 4
CB = 8
NCB = NB // CB

HALF = 32
CW = 256
WC = 512
NW = (7, 5)
WPW = WC // CW
NC = NW[0] * WPW
SKEW = 4
PIECE = 4


def attn_kernel(pos_hbm, scale_hbm, hid_hbm, w_hbm, k_hbm, v_hbm,
                mine_ref, other_ref, k_ref, v_ref,
                pos, scale, hid, cosf, sinf, x_s, wbuf, q_s, kv_s, psem, hsem, wsem, ksem, vsem):
    sp = lax.axis_index('sp')
    yy = sp // 2

    def first_of(c):
        return ((c + (NCB // 2) * (1 - yy)) % NCB) * CB

    def wcopy(j):
        return pltpu.make_async_copy(w_hbm.at[:, pl.ds(pl.multiple_of(j * WCOL, WCOL), WCOL)], wbuf.at[j % WSLOTS], wsem.at[j % WSLOTS])

    def kcopy(c):
        return pltpu.make_async_copy(k_hbm.at[pl.ds(first_of(c), CB)], k_ref.at[pl.ds(first_of(c), CB)], ksem.at[c])

    def vcopy(c):
        return pltpu.make_async_copy(v_hbm.at[pl.ds(first_of(c), CB)], v_ref.at[pl.ds(first_of(c), CB)], vsem.at[c])

    hcopy = pltpu.make_async_copy(hid_hbm, hid, hsem)
    hcopy.start()
    pcopy = pltpu.make_async_copy(pos_hbm, pos, psem.at[0])
    pcopy.start()
    scopy = pltpu.make_async_copy(scale_hbm, scale, psem.at[1])
    scopy.start()
    wcopy(0).start()
    pcopy.wait()
    wcopy(1).start()
    wcopy(2).start()

    lane8 = lax.broadcasted_iota(jnp.int32, (8, HD), 1)
    sub8 = lax.broadcasted_iota(jnp.int32, (8, HD), 0)
    inv_freq = jnp.exp((lane8 % (HD // 2)).astype(F32) * (-2.0 * math.log(500000.0) / HD))

    def angle_block(i, carry):
        p = jnp.zeros((8, HD), jnp.int32)
        for e in range(8):
            p = jnp.where(sub8 == e, pos[i * 8 + e], p)
        angles = p.astype(F32) * inv_freq
        rows = pl.ds(pl.multiple_of(i * 8, 8), 8)
        cosf[rows, :] = jnp.cos(angles)
        sin = jnp.sin(angles)
        sinf[rows, :] = jnp.where(lane8 < HD // 2, -sin, sin)
        return carry

    lax.fori_loop(0, NB // 8, angle_block, 0)
    q_s[...] = jnp.zeros_like(q_s)
    hcopy.wait()
    scopy.wait()
    wcopy(3).start()

    def norm_block(i, carry):
        rows = pl.ds(pl.multiple_of(i * 16, 16), 16)
        h = hid[rows, :].astype(F32)
        mean = jnp.mean(h, axis=-1, keepdims=True)
        cen = h - mean
        var = jnp.mean(cen * cen, axis=-1, keepdims=True)
        x_s[rows, :] = (cen * lax.rsqrt(var + 1e-5) * scale[...].astype(F32)[None, :]).astype(BF16)
        return carry

    lax.fori_loop(0, NB // 16, norm_block, 0)

    def rope(y):
        r = y * cosf[...] + pltpu.roll(y, HD // 2, 1) * sinf[...]
        return r.astype(BF16).astype(F32)

    def group(g, carry):
        for jj in range(4):
            j = g * 4 + jj
            wcopy(j).wait()
            acc = [jnp.dot(x_s[...], wbuf[j % WSLOTS, :, e * HD:(e + 1) * HD], preferred_element_type=F32) for e in range(2)]

            @pl.when(g == 0)
            def _():
                wcopy(j + WSLOTS).start()

            @pl.when(g == 1)
            def _():
                for c in range((0, 2, 4, 6)[jj], (2, 4, 6, 8)[jj]):
                    kcopy(c).start()
                    vcopy(c).start()

            y0, y1 = [jnp.clip(y.astype(BF16).astype(F32), -8.0, 8.0) for y in acc]
            if jj < 3:
                q_s[pl.ds(g * 8 + 2 * jj, NB, stride=16), :] = rope(y0)
                q_s[pl.ds(g * 8 + 2 * jj + 1, NB, stride=16), :] = rope(y1)
            else:
                kv_s[pl.ds(g, NB, stride=8), :] = rope(y0)
                kv_s[pl.ds(g + 2, NB, stride=8), :] = y1
        return carry

    lax.fori_loop(0, 2, group, 0)

    sub16 = lax.broadcasted_iota(jnp.int32, (16, HD), 0)
    col = lax.broadcasted_iota(jnp.int32, (16, ROWS), 1)
    row = lax.broadcasted_iota(jnp.int32, (16, ROWS), 0)
    parity_ok = (col % 2) == (row // 8)
    lane = lax.broadcasted_iota(jnp.int32, (16, HD), 1)

    def insert(b, r, cache, base_row):
        own = jnp.logical_and(r >= 0, r < SEQ_LOCAL)
        rc = jnp.clip(r, 0, SEQ_LOCAL - 1)
        start = pl.multiple_of((rc // 8) * 16, 16)
        sub = jnp.where(own, rc % 8, -1)
        n0 = kv_s[pl.ds(b * 8 + base_row, 1), :]
        n1 = kv_s[pl.ds(b * 8 + base_row + 1, 1), :]
        new = jnp.where(sub16 % 2 == 0, n0, n1)
        tile = cache[b, pl.ds(start, 16), :].astype(F32)
        cache[b, pl.ds(start, 16), :] = jnp.where(sub16 // 2 == sub, new, tile).astype(BF16)

    def chunk(c, out, m_acc, l_acc):
        kcopy(c).wait()
        vcopy(c).wait()

        b0 = first_of(c)
        for i in range(CB):
            r = pos[b0 + i] - sp * SEQ_LOCAL
            insert(b0 + i, r, k_ref, 0)
            insert(b0 + i, r, v_ref, 2)
        scores = []
        for i in range(CB):
            q = q_s[pl.ds(pl.multiple_of((b0 + i) * 16, 16), 16), :].astype(BF16)
            scores.append(lax.dot_general(q, k_ref[b0 + i], (((1,), (1,)), ((), ())), preferred_element_type=F32) * (HD ** -0.5))
        parts = []
        for i in range(CB):
            r = pos[b0 + i] - sp * SEQ_LOCAL
            s = jnp.where(jnp.logical_and(parity_ok, col < 2 * r + 2), scores[i], NEG)
            m = jnp.max(s, axis=1, keepdims=True)
            p = jnp.exp(s - m)
            parts.append((m, jnp.sum(p, axis=1, keepdims=True), p.astype(BF16)))
        for i in range(CB):
            m, l, p = parts[i]
            o = jnp.dot(p, v_ref[b0 + i], preferred_element_type=F32)
            bl = (c % (NCB // 2)) * CB + i
            out[pl.ds(bl, QPK, stride=HALF), :] = o[:QPK]
            out[pl.ds(QPK * HALF + bl, QPK, stride=HALF), :] = o[8:8 + QPK]
            m_acc = jnp.where(lane == bl, m, m_acc)
            l_acc = jnp.where(lane == bl, l, l_acc)
        return m_acc, l_acc

    for part, out in enumerate((other_ref, mine_ref)):
        zero = jnp.zeros((16, HD), F32)
        m_acc, l_acc = lax.fori_loop(part * (NCB // 2), (part + 1) * (NCB // 2), lambda c, st, out=out: chunk(c, out, *st), (zero, zero))
        block = jnp.concatenate([m_acc, l_acc, jnp.zeros((HD - 32, HD), F32)], axis=0)
        out[2 * QPK * HALF:(2 * QPK + 1) * HALF, :] = jnp.transpose(block)[:HALF]


def write_kernel(k_ref, v_ref, k_out, v_out, sem):
    copies = []
    for c in range(NCB):
        rows = pl.ds(c * CB, CB)
        copies.append(pltpu.make_async_copy(k_ref.at[rows], k_out.at[rows], sem.at[2 * c]))
        copies.append(pltpu.make_async_copy(v_ref.at[rows], v_out.at[rows], sem.at[2 * c + 1]))
    for c in copies:
        c.start()
    for c in copies:
        c.wait()


def merge_kernel(mine_in, other_in, hid_hbm, w_hbm, out,
                 hid, wbuf, om, oc, a_s, p_s, z1, a_z, z2, t_s, y_in, c_in, cy_in,
                 hsem, wsem, s1, r1, zs, zr, z2s, z2r, ts, ys, yr, cs, cr, cys, cyr):
    dp = lax.axis_index('dp')
    tp = lax.axis_index('tp')
    sp = lax.axis_index('sp')
    core = sp % 2
    yy = sp // 2
    partner = sp + 1 - 2 * core
    ynbr = sp + 2 - 4 * yy
    inner = jnp.logical_or(tp == 1, tp == 2)
    outer = jnp.logical_not(inner)
    n_inner = jnp.where(inner, 1, 0)
    z_in_nbr = jnp.where(tp < 2, jnp.where(tp == 0, 1, 2), jnp.where(tp == 3, 2, 1))
    z_out_nbr = jnp.where(tp < 2, 0, 3)
    nw = jnp.where(core == 1, NW[0], NW[1])
    nc = nw * WPW
    ncp = (NW[0] + NW[1]) * WPW - nc
    cols = jnp.where(core == 1, 0, NW[0] * WC)
    ocols = jnp.where(core == 1, NW[0] * WC, 0)

    def dev(t, s):
        return (dp, t, s)

    barrier = pltpu.get_barrier_semaphore()
    pl.semaphore_signal(barrier, inc=1, device_id=dev(tp, partner), device_id_type=MESH)
    pl.semaphore_signal(barrier, inc=1, device_id=dev(tp, ynbr), device_id_type=MESH)
    pl.semaphore_signal(barrier, inc=1, device_id=dev(z_in_nbr, sp), device_id_type=MESH)

    @pl.when(inner)
    def _():
        pl.semaphore_signal(barrier, inc=1, device_id=dev(z_out_nbr, sp), device_id_type=MESH)

    def wcopy(j):
        return pltpu.make_async_copy(w_hbm.at[:, pl.ds(pl.multiple_of(cols + j * WC, WC), WC)], wbuf.at[j], wsem.at[j])

    def wstart(j, carry):
        wcopy(j).start()
        return carry

    lax.fori_loop(0, nw, wstart, 0)
    hcopy = pltpu.make_async_copy(hid_hbm, hid, hsem)
    hcopy.start()

    def rcopy(src, dst, ssem, rsem, t, s):
        return pltpu.make_async_remote_copy(src_ref=src, dst_ref=dst, send_sem=ssem, recv_sem=rsem, device_id=dev(t, s), device_id_type=MESH)

    lane = lax.broadcasted_iota(jnp.int32, (HALF, HD), 1)
    heads = 2 * QPK
    pieces = [(i * PIECE, PIECE) for i in range(heads // PIECE)] + [(heads, 1)]
    ca = [rcopy(om.at[pl.ds(i, n)], oc.at[pl.ds(i, n)], s1.at[e], r1.at[e], tp, partner) for e, (i, n) in enumerate(pieces)]

    def factors(x, y):
        top = jnp.maximum(x, y)
        f0 = jnp.exp(x - top)
        f1 = jnp.exp(y - top)
        return top, f0, f1, f0 * pltpu.roll(x, HD - 16, 1) + f1 * pltpu.roll(y, HD - 16, 1)

    def column(f, h):
        e = h + 2 * (h // QPK)
        return f[:, e:e + 1]

    top, f0, f1, total = factors(mine_in[heads], other_in[heads])
    om[heads] = jnp.where(lane < 16, top, pltpu.roll(total, 16, 1))
    for h in range(heads):
        om[h] = mine_in[h] * column(f0, h) + other_in[h] * column(f1, h)
    pl.semaphore_wait(barrier, 3 + n_inner)
    for c in ca[::-1]:
        c.start()
    ca[-1].wait_recv()
    top, f0, f1, total = factors(om[heads], oc[heads])
    inv = 1.0 / total
    f0 = f0 * inv
    f1 = f1 * inv
    for e, (i, n) in reversed(list(enumerate(pieces[:-1]))):
        ca[e].wait_recv()
        for h in range(i, i + n):
            a_s[:, h * HD:(h + 1) * HD] = (om[h] * column(f0, h) + oc[h] * column(f1, h)).astype(BF16)

    def zc(j):
        return rcopy(p_s.at[j], z1.at[j], zs.at[j], zr.at[j], z_in_nbr, sp)

    def project(j, carry):
        wcopy(j).wait()
        for e in range(WC // 128):
            p = jnp.dot(a_s[...], wbuf[j, :, e * 128:(e + 1) * 128], preferred_element_type=F32)
            p_s[j * WPW + e * 128 // CW, :, (e * 128) % CW:(e * 128) % CW + 128] = p

        @pl.when(outer)
        def _():
            for e in range(WPW):
                zc(j * WPW + e).start()
        return carry

    lax.fori_loop(0, nw, project, 0)
    hcopy.wait()

    def mid(j):
        return rcopy(a_z.at[j], z2.at[j], z2s.at[j], z2r.at[j], z_in_nbr, sp)

    def back(j):
        return rcopy(t_s.at[j], z1.at[j], ts.at[j], zr.at[j], z_out_nbr, sp)

    def ycopy(src, j):
        return rcopy(src.at[j], y_in.at[j], ys.at[j], yr.at[j], tp, ynbr)

    def ccopy(src, j):
        return rcopy(src.at[j], c_in.at[j], cs.at[j], cr.at[j], tp, partner)

    def cycopy(j):
        return rcopy(y_in.at[j], cy_in.at[j], cys.at[j], cyr.at[j], tp, partner)

    def put(rows_start, col_start, j, val):
        rows = pl.ds(pl.multiple_of(rows_start, HALF), HALF)
        cl = pl.ds(pl.multiple_of(col_start + j * CW, CW), CW)
        out[rows, cl] = (hid[rows, cl].astype(F32) + val).astype(BF16)

    def e3(j):
        ycopy(t_s, j).wait_recv()
        cycopy(j).start()
        put((1 - yy) * HALF, cols, j, y_in[j])

    def e4(j):
        ccopy(t_s, j).wait_recv()
        put(yy * HALF, ocols, j, c_in[j])

    def e5(j):
        cycopy(j).wait_recv()
        put((1 - yy) * HALF, ocols, j, cy_in[j])

    def within(j, n, fn):
        @pl.when(jnp.logical_and(j >= 0, j < n))
        def _():
            fn(j)

    def tail(j, carry):
        e4(j)
        e5(j)
        return carry

    @pl.when(inner)
    def _():
        def e1(j):
            back(j).wait_recv()
            a_z[j] = p_s[j] + z1[j]
            mid(j).start()

        def e2(j):
            mid(j).wait_recv()
            t_s[j] = a_z[j] + z2[j]
            back(j).start()
            ycopy(t_s, j).start()
            ccopy(t_s, j).start()
            put(yy * HALF, cols, j, t_s[j])

        def step(t, carry):
            within(t, nc, e1)
            within(t - SKEW, nc, e2)
            within(t - 2 * SKEW, nc, e3)
            return carry

        lax.fori_loop(0, nc + 2 * SKEW, step, 0)
        lax.fori_loop(0, ncp, tail, 0)

        def drain(j, carry):
            mid(j).wait_send()
            back(j).wait_send()
            ycopy(t_s, j).wait_send()
            ccopy(t_s, j).wait_send()
            cycopy(j).wait_send()
            return carry

        lax.fori_loop(0, nc, drain, 0)

    @pl.when(outer)
    def _():
        def e1(j):
            zc(j).wait_recv()
            ycopy(z1, j).start()
            ccopy(z1, j).start()
            put(yy * HALF, cols, j, z1[j])

        def step(t, carry):
            within(t, nc, e1)
            within(t - SKEW, nc, e3)
            return carry

        lax.fori_loop(0, nc + SKEW, step, 0)
        lax.fori_loop(0, ncp, tail, 0)

        def drain(j, carry):
            zc(j).wait_send()
            ycopy(z1, j).wait_send()
            ccopy(z1, j).wait_send()
            cycopy(j).wait_send()
            return carry

        lax.fori_loop(0, nc, drain, 0)

    for c in ca:
        c.wait_send()


def solution(mesh):
    cache_spec = P('dp', 'sp', 'tp', None)
    any_spec = pl.BlockSpec(memory_space=pltpu.HBM)
    vmem_spec = pl.BlockSpec(memory_space=pltpu.VMEM)
    dma = pltpu.SemaphoreType.DMA

    def in_hbm(x):
        return pltpu.with_memory_space_constraint(x, pltpu.HBM)

    def local_step(hidden, norm_scale, w_qkv, w_out, k_cache, v_cache, positions):
        cache_shape = (NB, ROWS, HD)
        cache_out = jax.ShapeDtypeStruct(cache_shape, BF16)
        part = jax.ShapeDtypeStruct(((2 * QPK + 1) * HALF, HD), F32)
        cache_vmem = pltpu.VMEM(cache_shape, BF16)
        mine, other, k_vmem, v_vmem = pl.pallas_call(
            attn_kernel,
            out_shape=(part, part, cache_vmem, cache_vmem),
            in_specs=[any_spec] * 6,
            out_specs=(vmem_spec,) * 4,
            scratch_shapes=[
                pltpu.SMEM((NB,), jnp.int32),
                pltpu.VMEM((D,), BF16),
                pltpu.VMEM((NB, D), BF16),
                pltpu.VMEM((NB, HD), F32),
                pltpu.VMEM((NB, HD), F32),
                pltpu.VMEM((NB, D), BF16),
                pltpu.VMEM((WSLOTS, D, WCOL), BF16),
                pltpu.VMEM((16 * NB, HD), F32),
                pltpu.VMEM((8 * NB, HD), F32),
                dma((2,)), dma(()), dma((WSLOTS,)), dma((NCB,)), dma((NCB,)),
            ],
            compiler_params=pltpu.CompilerParams(vmem_limit_bytes=24 << 20),
            name='qkv_attention',
        )(in_hbm(positions), in_hbm(norm_scale), in_hbm(hidden), in_hbm(w_qkv), in_hbm(k_cache.reshape(cache_shape)), in_hbm(v_cache.reshape(cache_shape)))

        sps = mesh.shape['sp']
        other = lax.ppermute(other, 'sp', [(i, (i + sps // 2) % sps) for i in range(sps)])
        k_new, v_new = pl.pallas_call(
            write_kernel,
            out_shape=(cache_out, cache_out),
            in_specs=[vmem_spec] * 2,
            out_specs=(any_spec,) * 2,
            scratch_shapes=[dma((2 * NCB,))],
            compiler_params=pltpu.CompilerParams(vmem_limit_bytes=4 << 20),
            cost_estimate=pl.CostEstimate(flops=20_000_000_000, bytes_accessed=32 << 20, transcendentals=0),
            name='cache_write',
        )(k_vmem, v_vmem)

        heads = (2 * QPK + 1, HALF, HD)
        chunk = (NC, HALF, CW)
        h_out = pl.pallas_call(
            merge_kernel,
            out_shape=jax.ShapeDtypeStruct((NB, D), BF16),
            in_specs=[vmem_spec, vmem_spec, any_spec, any_spec],
            out_specs=vmem_spec,
            scratch_shapes=[
                pltpu.VMEM((NB, D), BF16),
                pltpu.VMEM((NW[0], 2 * QPK * HD, WC), BF16),
                pltpu.VMEM(heads, F32),
                pltpu.VMEM(heads, F32),
                pltpu.VMEM((HALF, 2 * QPK * HD), BF16),
            ] + [pltpu.VMEM(chunk, F32)] * 8 + [
                dma(()), dma((NW[0],)), dma((2 * QPK // PIECE + 1,)), dma((2 * QPK // PIECE + 1,)),
            ] + [dma((NC,))] * 11,
            compiler_params=pltpu.CompilerParams(collective_id=0, has_side_effects=True, vmem_limit_bytes=32 << 20),
            name='merge_project',
        )(mine.reshape(heads), other.reshape(heads), in_hbm(hidden), in_hbm(w_out))
        return h_out, k_new.reshape(k_cache.shape), v_new.reshape(v_cache.shape)

    return jax.shard_map(
        local_step,
        mesh=mesh,
        in_specs=(P('dp', None), P(None), P(None, 'tp'), P('tp', None), cache_spec, cache_spec, P('dp')),
        out_specs=(P('dp', None), cache_spec, cache_spec),
        check_vma=False,
    )
```

```python
import math
import jax
import jax.numpy as jnp
from jax import lax
from jax.experimental import pallas as pl
from jax.experimental.pallas import tpu as pltpu
from jax.sharding import PartitionSpec as P

F32 = jnp.float32
BF16 = jnp.bfloat16
MESH = pl.DeviceIdType.MESH

NB = 64
D = 6144
HD = 128
SEQ_LOCAL = 256
ROWS = 2 * SEQ_LOCAL
QPK = 6
NEG = -1e30

WCOL = 256
WSLOTS = 4
CB = 16
NCB = NB // CB

HALF = 32
CW = 256
WC = 512
NW = (7, 5)
WPW = WC // CW
NC = NW[0] * WPW
SKEW = 4
PIECE = 4


def attn_kernel(pos_hbm, scale_hbm, hid_hbm, w_hbm, k_hbm, v_hbm,
                mine_ref, other_ref, k_ref, v_ref,
                pos, scale, hid, cosf, sinf, x_s, wbuf, q_s, kv_s, psem, hsem, wsem, ksem, vsem):
    sp = lax.axis_index('sp')
    yy = sp // 2

    def first_of(c):
        return ((c + (NCB // 2) * (1 - yy)) % NCB) * CB

    def wcopy(j):
        return pltpu.make_async_copy(w_hbm.at[:, pl.ds(pl.multiple_of(j * WCOL, WCOL), WCOL)], wbuf.at[j % WSLOTS], wsem.at[j % WSLOTS])

    def kcopy(c):
        return pltpu.make_async_copy(k_hbm.at[pl.ds(first_of(c), CB)], k_ref.at[pl.ds(first_of(c), CB)], ksem.at[c])

    def vcopy(c):
        return pltpu.make_async_copy(v_hbm.at[pl.ds(first_of(c), CB)], v_ref.at[pl.ds(first_of(c), CB)], vsem.at[c])

    hcopy = pltpu.make_async_copy(hid_hbm, hid, hsem)
    hcopy.start()
    pcopy = pltpu.make_async_copy(pos_hbm, pos, psem.at[0])
    pcopy.start()
    scopy = pltpu.make_async_copy(scale_hbm, scale, psem.at[1])
    scopy.start()
    wcopy(0).start()
    pcopy.wait()
    wcopy(1).start()
    wcopy(2).start()

    lane8 = lax.broadcasted_iota(jnp.int32, (8, HD), 1)
    sub8 = lax.broadcasted_iota(jnp.int32, (8, HD), 0)
    inv_freq = jnp.exp((lane8 % (HD // 2)).astype(F32) * (-2.0 * math.log(500000.0) / HD))

    def angle_block(i, carry):
        p = jnp.zeros((8, HD), jnp.int32)
        for e in range(8):
            p = jnp.where(sub8 == e, pos[i * 8 + e], p)
        angles = p.astype(F32) * inv_freq
        rows = pl.ds(pl.multiple_of(i * 8, 8), 8)
        cosf[rows, :] = jnp.cos(angles)
        sin = jnp.sin(angles)
        sinf[rows, :] = jnp.where(lane8 < HD // 2, -sin, sin)
        return carry

    lax.fori_loop(0, NB // 8, angle_block, 0)
    q_s[...] = jnp.zeros_like(q_s)
    hcopy.wait()
    scopy.wait()
    wcopy(3).start()

    def norm_block(i, carry):
        rows = pl.ds(pl.multiple_of(i * 16, 16), 16)
        h = hid[rows, :].astype(F32)
        mean = jnp.mean(h, axis=-1, keepdims=True)
        cen = h - mean
        var = jnp.mean(cen * cen, axis=-1, keepdims=True)
        x_s[rows, :] = (cen * lax.rsqrt(var + 1e-5) * scale[...].astype(F32)[None, :]).astype(BF16)
        return carry

    lax.fori_loop(0, NB // 16, norm_block, 0)

    def rope(y):
        r = y * cosf[...] + pltpu.roll(y, HD // 2, 1) * sinf[...]
        return r.astype(BF16).astype(F32)

    def group(g, carry):
        for jj in range(4):
            j = g * 4 + jj
            wcopy(j).wait()
            acc = [jnp.dot(x_s[...], wbuf[j % WSLOTS, :, e * HD:(e + 1) * HD], preferred_element_type=F32) for e in range(2)]

            @pl.when(g == 0)
            def _():
                wcopy(j + WSLOTS).start()

            @pl.when(g == 1)
            def _():
                for c in range((0, 1, 2, 3)[jj], (1, 2, 3, 4)[jj]):
                    kcopy(c).start()
                    vcopy(c).start()

            y0, y1 = [jnp.clip(y.astype(BF16).astype(F32), -8.0, 8.0) for y in acc]
            if jj < 3:
                q_s[pl.ds(g * 8 + 2 * jj, NB, stride=16), :] = rope(y0)
                q_s[pl.ds(g * 8 + 2 * jj + 1, NB, stride=16), :] = rope(y1)
            else:
                kv_s[pl.ds(g, NB, stride=8), :] = rope(y0)
                kv_s[pl.ds(g + 2, NB, stride=8), :] = y1
        return carry

    lax.fori_loop(0, 2, group, 0)

    sub16 = lax.broadcasted_iota(jnp.int32, (16, HD), 0)
    col = lax.broadcasted_iota(jnp.int32, (16, ROWS), 1)
    row = lax.broadcasted_iota(jnp.int32, (16, ROWS), 0)
    parity_ok = (col % 2) == (row // 8)
    lane = lax.broadcasted_iota(jnp.int32, (16, HD), 1)

    def insert(b, r, cache, base_row):
        own = jnp.logical_and(r >= 0, r < SEQ_LOCAL)
        rc = jnp.clip(r, 0, SEQ_LOCAL - 1)
        start = pl.multiple_of((rc // 8) * 16, 16)
        sub = jnp.where(own, rc % 8, -1)
        n0 = kv_s[pl.ds(b * 8 + base_row, 1), :]
        n1 = kv_s[pl.ds(b * 8 + base_row + 1, 1), :]
        new = jnp.where(sub16 % 2 == 0, n0, n1)
        tile = cache[b, pl.ds(start, 16), :].astype(F32)
        cache[b, pl.ds(start, 16), :] = jnp.where(sub16 // 2 == sub, new, tile).astype(BF16)

    def chunk(c, out, m_acc, l_acc):
        kcopy(c).wait()
        vcopy(c).wait()

        b0 = first_of(c)
        for i in range(CB):
            r = pos[b0 + i] - sp * SEQ_LOCAL
            insert(b0 + i, r, k_ref, 0)
            insert(b0 + i, r, v_ref, 2)
        scores = []
        for i in range(CB):
            q = q_s[pl.ds(pl.multiple_of((b0 + i) * 16, 16), 16), :].astype(BF16)
            scores.append(lax.dot_general(q, k_ref[b0 + i], (((1,), (1,)), ((), ())), preferred_element_type=F32) * (HD ** -0.5))
        parts = []
        for i in range(CB):
            r = pos[b0 + i] - sp * SEQ_LOCAL
            s = jnp.where(jnp.logical_and(parity_ok, col < 2 * r + 2), scores[i], NEG)
            m = jnp.max(s, axis=1, keepdims=True)
            p = jnp.exp(s - m)
            parts.append((m, jnp.sum(p, axis=1, keepdims=True), p.astype(BF16)))
        for i in range(CB):
            m, l, p = parts[i]
            o = jnp.dot(p, v_ref[b0 + i], preferred_element_type=F32)
            bl = (c % (NCB // 2)) * CB + i
            out[pl.ds(bl, QPK, stride=HALF), :] = o[:QPK]
            out[pl.ds(QPK * HALF + bl, QPK, stride=HALF), :] = o[8:8 + QPK]
            m_acc = jnp.where(lane == bl, m, m_acc)
            l_acc = jnp.where(lane == bl, l, l_acc)
        return m_acc, l_acc

    for part, out in enumerate((other_ref, mine_ref)):
        zero = jnp.zeros((16, HD), F32)
        m_acc, l_acc = lax.fori_loop(part * (NCB // 2), (part + 1) * (NCB // 2), lambda c, st, out=out: chunk(c, out, *st), (zero, zero))
        block = jnp.concatenate([m_acc, l_acc, jnp.zeros((HD - 32, HD), F32)], axis=0)
        out[2 * QPK * HALF:(2 * QPK + 1) * HALF, :] = jnp.transpose(block)[:HALF]


def write_kernel(k_ref, v_ref, k_out, v_out, sem):
    copies = []
    for c in range(NCB):
        rows = pl.ds(c * CB, CB)
        copies.append(pltpu.make_async_copy(k_ref.at[rows], k_out.at[rows], sem.at[2 * c]))
        copies.append(pltpu.make_async_copy(v_ref.at[rows], v_out.at[rows], sem.at[2 * c + 1]))
    for c in copies:
        c.start()
    for c in copies:
        c.wait()


def merge_kernel(mine_in, other_in, hid_hbm, w_hbm, out,
                 hid, wbuf, om, oc, a_s, p_s, z1, a_z, z2, t_s, y_in, c_in, cy_in,
                 hsem, wsem, s1, r1, zs, zr, z2s, z2r, ts, ys, yr, cs, cr, cys, cyr):
    dp = lax.axis_index('dp')
    tp = lax.axis_index('tp')
    sp = lax.axis_index('sp')
    core = sp % 2
    yy = sp // 2
    partner = sp + 1 - 2 * core
    ynbr = sp + 2 - 4 * yy
    inner = jnp.logical_or(tp == 1, tp == 2)
    outer = jnp.logical_not(inner)
    n_inner = jnp.where(inner, 1, 0)
    z_in_nbr = jnp.where(tp < 2, jnp.where(tp == 0, 1, 2), jnp.where(tp == 3, 2, 1))
    z_out_nbr = jnp.where(tp < 2, 0, 3)
    nw = jnp.where(core == 1, NW[0], NW[1])
    nc = nw * WPW
    ncp = (NW[0] + NW[1]) * WPW - nc
    cols = jnp.where(core == 1, 0, NW[0] * WC)
    ocols = jnp.where(core == 1, NW[0] * WC, 0)

    def dev(t, s):
        return (dp, t, s)

    barrier = pltpu.get_barrier_semaphore()
    pl.semaphore_signal(barrier, inc=1, device_id=dev(tp, partner), device_id_type=MESH)
    pl.semaphore_signal(barrier, inc=1, device_id=dev(tp, ynbr), device_id_type=MESH)
    pl.semaphore_signal(barrier, inc=1, device_id=dev(z_in_nbr, sp), device_id_type=MESH)

    @pl.when(inner)
    def _():
        pl.semaphore_signal(barrier, inc=1, device_id=dev(z_out_nbr, sp), device_id_type=MESH)

    def wcopy(j):
        return pltpu.make_async_copy(w_hbm.at[:, pl.ds(pl.multiple_of(cols + j * WC, WC), WC)], wbuf.at[j], wsem.at[j])

    def wstart(j, carry):
        wcopy(j).start()
        return carry

    lax.fori_loop(0, nw, wstart, 0)
    hcopy = pltpu.make_async_copy(hid_hbm, hid, hsem)
    hcopy.start()

    def rcopy(src, dst, ssem, rsem, t, s):
        return pltpu.make_async_remote_copy(src_ref=src, dst_ref=dst, send_sem=ssem, recv_sem=rsem, device_id=dev(t, s), device_id_type=MESH)

    lane = lax.broadcasted_iota(jnp.int32, (HALF, HD), 1)
    heads = 2 * QPK
    pieces = [(i * PIECE, PIECE) for i in range(heads // PIECE)] + [(heads, 1)]
    ca = [rcopy(om.at[pl.ds(i, n)], oc.at[pl.ds(i, n)], s1.at[e], r1.at[e], tp, partner) for e, (i, n) in enumerate(pieces)]

    def factors(x, y):
        top = jnp.maximum(x, y)
        f0 = jnp.exp(x - top)
        f1 = jnp.exp(y - top)
        return top, f0, f1, f0 * pltpu.roll(x, HD - 16, 1) + f1 * pltpu.roll(y, HD - 16, 1)

    def column(f, h):
        e = h + 2 * (h // QPK)
        return f[:, e:e + 1]

    top, f0, f1, total = factors(mine_in[heads], other_in[heads])
    om[heads] = jnp.where(lane < 16, top, pltpu.roll(total, 16, 1))
    for h in range(heads):
        om[h] = mine_in[h] * column(f0, h) + other_in[h] * column(f1, h)
    pl.semaphore_wait(barrier, 3 + n_inner)
    for c in ca[::-1]:
        c.start()
    ca[-1].wait_recv()
    top, f0, f1, total = factors(om[heads], oc[heads])
    inv = 1.0 / total
    f0 = f0 * inv
    f1 = f1 * inv
    for e, (i, n) in reversed(list(enumerate(pieces[:-1]))):
        ca[e].wait_recv()
        for h in range(i, i + n):
            a_s[:, h * HD:(h + 1) * HD] = (om[h] * column(f0, h) + oc[h] * column(f1, h)).astype(BF16)

    def zc(j):
        return rcopy(p_s.at[j], z1.at[j], zs.at[j], zr.at[j], z_in_nbr, sp)

    def project(j, carry):
        wcopy(j).wait()
        for e in range(WC // 128):
            p = jnp.dot(a_s[...], wbuf[j, :, e * 128:(e + 1) * 128], preferred_element_type=F32)
            p_s[j * WPW + e * 128 // CW, :, (e * 128) % CW:(e * 128) % CW + 128] = p

        @pl.when(outer)
        def _():
            for e in range(WPW):
                zc(j * WPW + e).start()
        return carry

    lax.fori_loop(0, nw, project, 0)
    hcopy.wait()

    def mid(j):
        return rcopy(a_z.at[j], z2.at[j], z2s.at[j], z2r.at[j], z_in_nbr, sp)

    def back(j):
        return rcopy(t_s.at[j], z1.at[j], ts.at[j], zr.at[j], z_out_nbr, sp)

    def ycopy(src, j):
        return rcopy(src.at[j], y_in.at[j], ys.at[j], yr.at[j], tp, ynbr)

    def ccopy(src, j):
        return rcopy(src.at[j], c_in.at[j], cs.at[j], cr.at[j], tp, partner)

    def cycopy(j):
        return rcopy(y_in.at[j], cy_in.at[j], cys.at[j], cyr.at[j], tp, partner)

    def put(rows_start, col_start, j, val):
        rows = pl.ds(pl.multiple_of(rows_start, HALF), HALF)
        cl = pl.ds(pl.multiple_of(col_start + j * CW, CW), CW)
        out[rows, cl] = (hid[rows, cl].astype(F32) + val).astype(BF16)

    def e3(j):
        ycopy(t_s, j).wait_recv()
        cycopy(j).start()
        put((1 - yy) * HALF, cols, j, y_in[j])

    def e4(j):
        ccopy(t_s, j).wait_recv()
        put(yy * HALF, ocols, j, c_in[j])

    def e5(j):
        cycopy(j).wait_recv()
        put((1 - yy) * HALF, ocols, j, cy_in[j])

    def within(j, n, fn):
        @pl.when(jnp.logical_and(j >= 0, j < n))
        def _():
            fn(j)

    def tail(j, carry):
        e4(j)
        e5(j)
        return carry

    @pl.when(inner)
    def _():
        def e1(j):
            back(j).wait_recv()
            a_z[j] = p_s[j] + z1[j]
            mid(j).start()

        def e2(j):
            mid(j).wait_recv()
            t_s[j] = a_z[j] + z2[j]
            back(j).start()
            ycopy(t_s, j).start()
            ccopy(t_s, j).start()
            put(yy * HALF, cols, j, t_s[j])

        def step(t, carry):
            within(t, nc, e1)
            within(t - SKEW, nc, e2)
            within(t - 2 * SKEW, nc, e3)
            return carry

        lax.fori_loop(0, nc + 2 * SKEW, step, 0)
        lax.fori_loop(0, ncp, tail, 0)

        def drain(j, carry):
            mid(j).wait_send()
            back(j).wait_send()
            ycopy(t_s, j).wait_send()
            ccopy(t_s, j).wait_send()
            cycopy(j).wait_send()
            return carry

        lax.fori_loop(0, nc, drain, 0)

    @pl.when(outer)
    def _():
        def e1(j):
            zc(j).wait_recv()
            ycopy(z1, j).start()
            ccopy(z1, j).start()
            put(yy * HALF, cols, j, z1[j])

        def step(t, carry):
            within(t, nc, e1)
            within(t - SKEW, nc, e3)
            return carry

        lax.fori_loop(0, nc + SKEW, step, 0)
        lax.fori_loop(0, ncp, tail, 0)

        def drain(j, carry):
            zc(j).wait_send()
            ycopy(z1, j).wait_send()
            ccopy(z1, j).wait_send()
            cycopy(j).wait_send()
            return carry

        lax.fori_loop(0, nc, drain, 0)

    for c in ca:
        c.wait_send()


def solution(mesh):
    cache_spec = P('dp', 'sp', 'tp', None)
    any_spec = pl.BlockSpec(memory_space=pltpu.HBM)
    vmem_spec = pl.BlockSpec(memory_space=pltpu.VMEM)
    dma = pltpu.SemaphoreType.DMA

    def in_hbm(x):
        return pltpu.with_memory_space_constraint(x, pltpu.HBM)

    def local_step(hidden, norm_scale, w_qkv, w_out, k_cache, v_cache, positions):
        cache_shape = (NB, ROWS, HD)
        cache_out = jax.ShapeDtypeStruct(cache_shape, BF16)
        part = jax.ShapeDtypeStruct(((2 * QPK + 1) * HALF, HD), F32)
        cache_vmem = pltpu.VMEM(cache_shape, BF16)
        mine, other, k_vmem, v_vmem = pl.pallas_call(
            attn_kernel,
            out_shape=(part, part, cache_vmem, cache_vmem),
            in_specs=[any_spec] * 6,
            out_specs=(vmem_spec,) * 4,
            scratch_shapes=[
                pltpu.SMEM((NB,), jnp.int32),
                pltpu.VMEM((D,), BF16),
                pltpu.VMEM((NB, D), BF16),
                pltpu.VMEM((NB, HD), F32),
                pltpu.VMEM((NB, HD), F32),
                pltpu.VMEM((NB, D), BF16),
                pltpu.VMEM((WSLOTS, D, WCOL), BF16),
                pltpu.VMEM((16 * NB, HD), F32),
                pltpu.VMEM((8 * NB, HD), F32),
                dma((2,)), dma(()), dma((WSLOTS,)), dma((NCB,)), dma((NCB,)),
            ],
            compiler_params=pltpu.CompilerParams(vmem_limit_bytes=24 << 20),
            name='qkv_attention',
        )(in_hbm(positions), in_hbm(norm_scale), in_hbm(hidden), in_hbm(w_qkv), in_hbm(k_cache.reshape(cache_shape)), in_hbm(v_cache.reshape(cache_shape)))

        sps = mesh.shape['sp']
        other = lax.ppermute(other, 'sp', [(i, (i + sps // 2) % sps) for i in range(sps)])
        k_new, v_new = pl.pallas_call(
            write_kernel,
            out_shape=(cache_out, cache_out),
            in_specs=[vmem_spec] * 2,
            out_specs=(any_spec,) * 2,
            scratch_shapes=[dma((2 * NCB,))],
            compiler_params=pltpu.CompilerParams(vmem_limit_bytes=4 << 20),
            cost_estimate=pl.CostEstimate(flops=20_000_000_000, bytes_accessed=32 << 20, transcendentals=0),
            name='cache_write',
        )(k_vmem, v_vmem)

        heads = (2 * QPK + 1, HALF, HD)
        chunk = (NC, HALF, CW)
        h_out = pl.pallas_call(
            merge_kernel,
            out_shape=jax.ShapeDtypeStruct((NB, D), BF16),
            in_specs=[vmem_spec, vmem_spec, any_spec, any_spec],
            out_specs=vmem_spec,
            scratch_shapes=[
                pltpu.VMEM((NB, D), BF16),
                pltpu.VMEM((NW[0], 2 * QPK * HD, WC), BF16),
                pltpu.VMEM(heads, F32),
                pltpu.VMEM(heads, F32),
                pltpu.VMEM((HALF, 2 * QPK * HD), BF16),
            ] + [pltpu.VMEM(chunk, F32)] * 8 + [
                dma(()), dma((NW[0],)), dma((2 * QPK // PIECE + 1,)), dma((2 * QPK // PIECE + 1,)),
            ] + [dma((NC,))] * 11,
            compiler_params=pltpu.CompilerParams(collective_id=0, has_side_effects=True, vmem_limit_bytes=32 << 20),
            name='merge_project',
        )(mine.reshape(heads), other.reshape(heads), in_hbm(hidden), in_hbm(w_out))
        return h_out, k_new.reshape(k_cache.shape), v_new.reshape(v_cache.shape)

    return jax.shard_map(
        local_step,
        mesh=mesh,
        in_specs=(P('dp', None), P(None), P(None, 'tp'), P('tp', None), cache_spec, cache_spec, P('dp')),
        out_specs=(P('dp', None), cache_spec, cache_spec),
        check_vma=False,
    )
```
